32 devices in a mesh: rep: 8 (over y, x, core), tp: 4 (over z).
Axes of the slice: x: 2, y: 2, z: 4, core: 2. Of those that a mesh axis runs over, the one named last changes fastest.
Arguments:
- residual_in: bfloat16 [8, 512, 8192], P('rep', 'tp'), may hold values from -6 to 6
- norm_gain: bfloat16 [8192], replicated, may hold values from 0.099609375 to 1.8984375
- w_query: bfloat16 [8192, 4096], P(None, 'tp'), may hold values from -1 to 1
- w_keyval: bfloat16 [8192, 1024], P(None, 'tp'), may hold values from -0.0625 to 0.0625
- w_out: bfloat16 [4096, 8192], P('tp'), may hold values from -0.375 to 0.375
- score_head: bfloat16 [8192], replicated, may hold values from -0.0625 to 0.0625
- lengths: int32 [8], P('rep'), may hold values from 256 to 512
- policy_slots: bfloat16 [8, 768, 8192], P('rep', None, 'tp'), may hold values from -6 to 6
Outputs:
- scored_hidden: bfloat16 [8, 512, 8192], P('rep', 'tp')
- rewards: float32 [8], P('rep')
- policy_copies: bfloat16 [8, 768, 8192], P('rep', None, 'tp')
The draws below stay inside these ranges and needn't reach their ends.
All inputs are finite; a program needn't handle non-finite values.
Results may differ from the reference program's by a relative error of at most 0.017.
The reference program's roundings to bfloat16 on the way count: a program that leaves them out, or rounds other values in their place, can miss the bound.
Values may be sent and summed in bfloat16 or wider, within the bound.
A program may use at most 128 MiB of HBM per device.

```python
import jax
import jax.numpy as jnp
from jax import lax

D = 8192
QH = 32
KVH = 4
HS = 128
LEN = 512
PROWS = 768
QW = 4096
KW = 512
REPLICAS = 8
N_TP = 4


def draw_w_query(key, part):
    values = jax.random.normal(jax.random.fold_in(key, 11), (D, QW), jnp.float32) * D ** (-0.5)
    return jnp.clip(values, -1.0, 1.0).astype(jnp.bfloat16)


def with_ends(result, own_key, low, largest):
    longest = result.shape.index(max(result.shape))
    spots = []
    for shift in (0, 1):
        where = [jax.random.randint(jax.random.fold_in(own_key, axis), (), 0, length) for axis, length in enumerate(result.shape)]
        where[longest] = (where[longest] + shift) % result.shape[longest]
        spots.append(tuple(where))
    return result.at[spots[0]].set(low).at[spots[1]].set(largest)


def block_levels(rng, dims, pieces, least, largest):
    gain, own = 1.0, jax.random.fold_in(rng, 6)
    for position, blocks in pieces:
        draws = jnp.exp(jax.random.uniform(jax.random.fold_in(own, position), (blocks,), jnp.float32, least / len(pieces), largest / len(pieces)))
        gain = gain * jnp.repeat(draws, dims[position] // blocks).reshape([-1 if axis == position else 1 for axis in range(len(dims))])
    return gain


def centred(rng, dims, deviation, bound, cuts=(), held_as=jnp.bfloat16):
    result = jax.random.normal(rng, dims, jnp.float32) * deviation
    if len(cuts) > 0:
        result = block_levels(rng, dims, cuts, -0.22, 0.18) * result
    return jnp.clip(result, min=-bound, max=bound).astype(held_as)


def setup_inputs(seed: int = 0) -> dict:
    arg_keys = jax.random.split(jax.random.key(seed), 9)
    residual_in = centred(arg_keys[0], (REPLICAS, LEN, D), 1.0, 6.0, ((0, 8), (1, 4)))
    norm_gain = jnp.clip(1.0 + 0.18 * jax.random.normal(arg_keys[1], (D,), jnp.float32), 0.099609375, 1.8984375).astype(jnp.bfloat16)
    w_query = draw_w_query(jax.random.fold_in(arg_keys[8], 71), 0)
    w_keyval = centred(arg_keys[3], (D, 2 * KW), D ** -0.5, 0.0625, ((1, 4),))
    w_out = centred(arg_keys[4], (QW, D), (QW // 16) ** -0.5, 0.375, ((0, 4),))
    score_head = centred(arg_keys[5], (D,), D ** -0.5, 0.0625)
    lengths = with_ends(jax.random.randint(arg_keys[6], (REPLICAS,), LEN // 2, LEN + 1), jax.random.fold_in(arg_keys[6], 1), LEN // 2, LEN).astype(jnp.int32)
    policy_slots = centred(arg_keys[7], (REPLICAS, PROWS, D), 1.0, 6.0, ((0, 8), (2, 4)))
    return dict(residual_in=residual_in, norm_gain=norm_gain, w_query=w_query, w_keyval=w_keyval, w_out=w_out, score_head=score_head, lengths=lengths, policy_slots=policy_slots)


def one_rollout(residual_row, length, norm_gain, w_query, w_keyval, w_out, score_head):
    resid = residual_row.astype(jnp.float32)
    meansq = lax.optimization_barrier(jnp.mean(resid * resid, axis=-1, keepdims=True))
    normed = (resid * lax.rsqrt(meansq + 1e-05) * norm_gain.astype(jnp.float32)).astype(jnp.bfloat16)
    queries = jnp.dot(normed, w_query, preferred_element_type=jnp.float32).astype(jnp.bfloat16)
    keyvals = jnp.dot(normed, w_keyval, preferred_element_type=jnp.float32).astype(jnp.bfloat16)
    group = QH // KVH
    qheads = queries.reshape(LEN, QH, HS).transpose(1, 0, 2).astype(jnp.float32)
    kheads = keyvals[:, :KW].reshape(LEN, KVH, HS).transpose(1, 0, 2)
    vheads = keyvals[:, KW:].reshape(LEN, KVH, HS).transpose(1, 0, 2)
    kheads = jnp.repeat(kheads, group, axis=0).astype(jnp.float32)
    vheads = jnp.repeat(vheads, group, axis=0).astype(jnp.float32)
    scores = jnp.einsum('hqd,hkd->hqk', qheads, kheads) * HS ** (-0.5)
    rowpos = jnp.arange(LEN, dtype=jnp.int32)[:, None]
    colpos = jnp.arange(LEN, dtype=jnp.int32)[None, :]
    valid = (colpos <= rowpos) & (colpos < length)
    scores = jnp.where(valid[None], scores, -1e+30)
    probs = jax.nn.softmax(scores, axis=-1).astype(jnp.bfloat16)
    attended = jnp.einsum('hqk,hkd->hqd', probs.astype(jnp.float32), vheads).astype(jnp.bfloat16)
    attended = attended.transpose(1, 0, 2).reshape(LEN, QW)
    groups = attended.reshape(LEN, N_TP, QW // N_TP).astype(jnp.float32)
    wgroups = w_out.reshape(N_TP, QW // N_TP, D).astype(jnp.float32)
    partial_value = jnp.einsum('lti,tid->tld', groups, wgroups).astype(jnp.bfloat16)
    partial_value = lax.optimization_barrier(partial_value)
    summed = lax.optimization_barrier(jnp.sum(partial_value.astype(jnp.float32), axis=0))
    hidden = (resid + summed).astype(jnp.bfloat16)
    head = score_head.astype(jnp.float32)
    last_row = lax.dynamic_slice_in_dim(hidden, (length - 1).astype(jnp.int32), 1, 0)[0]
    reward = jnp.sum(last_row.astype(jnp.float32) * head)
    pooled = jnp.sum(hidden.astype(jnp.float32) * head[None, :]) * LEN ** (-0.5)
    return (hidden, reward + pooled)

def reference(residual_in, norm_gain, w_query, w_keyval, w_out, score_head, lengths, policy_slots):

    def step(pair):
        return one_rollout(pair[0], pair[1], norm_gain, w_query, w_keyval, w_out, score_head)
    scored_hidden, rewards = lax.map(step, (residual_in, lengths.astype(jnp.int32)))
    policy_copies = jnp.broadcast_to(policy_slots[0:1], policy_slots.shape)
    return (scored_hidden, rewards.astype(jnp.float32), policy_copies)
```

```python
import functools

import jax
import jax.numpy as jnp
from jax import lax
from jax.experimental import pallas as pl
from jax.experimental.pallas import tpu as pltpu
from jax.sharding import PartitionSpec as P

QH = 32
KVH = 4
HS = 128
MESH = pl.DeviceIdType.MESH
F32 = jnp.float32
BF16 = jnp.bfloat16
CHUNKS = 16
LAG = 2


def kernel(
    n, R, kvw, heads,
    resid_h, gain, wq_h, wkv_h, wo_h, head, lens, pol_in,
    out_h, rew, pol_out,
    wq, wkv, wo, resid, nrm, part, qs, accq, acckv, kvown, kvin, kf, vf, att, rmy, rin,
    load_sem, ag_send, ag_recv, rs_send, rs_recv, kv_send, kv_recv, r_send, r_recv, p_send, p_recv, p_loc, out_sem,
):
    t = lax.axis_index("tp")
    r = lax.axis_index("rep")
    C = nrm.shape[1]
    rows, cols = nrm.shape[2], nrm.shape[3]
    seq = n * rows
    length = lens[0]

    def chunk_of(ref, c):
        return ref.at[:, pl.ds(pl.multiple_of(c * cols, cols), cols)]

    loads = [pltpu.make_async_copy(chunk_of(resid_h.at[0], c), resid.at[c], load_sem.at[c]) for c in range(C)]
    wloads = [
        pltpu.make_async_copy(wq_h, wq, load_sem.at[C]),
        pltpu.make_async_copy(wkv_h, wkv, load_sem.at[C + 1]),
    ]
    oloads = [pltpu.make_async_copy(chunk_of(wo_h, c), wo.at[c], load_sem.at[C + 2 + c]) for c in range(C)]
    for cp in loads + wloads + oloads:
        cp.start()
    kf[...] = jnp.zeros_like(kf)
    vf[...] = jnp.zeros_like(vf)

    barrier = pltpu.get_barrier_semaphore()
    for k in range(1, n):
        pl.semaphore_signal(barrier, inc=1, device_id={"tp": lax.rem(t + k, n)}, device_id_type=MESH)
    for k in range(1, R):
        pl.semaphore_signal(barrier, inc=1, device_id={"rep": lax.rem(r + k, R)}, device_id_type=MESH)

    for cp in loads:
        cp.wait()

    def sq(c, acc):
        x = resid[c].astype(F32)
        return acc + jnp.sum(x * x, axis=1, keepdims=True)

    ms = lax.fori_loop(0, C, sq, jnp.zeros((rows, 1), F32))
    scale = lax.rsqrt(ms / (C * cols) + 1e-05)

    def norm(c, carry):
        nrm[t, c] = (resid[c].astype(F32) * scale * gain[c].astype(F32)).astype(BF16)
        return carry

    lax.fori_loop(0, C, norm, 0)
    pl.semaphore_wait(barrier, n - 1 + R - 1)

    steps = R.bit_length() - 1

    def pol(src, s):
        return pltpu.make_async_remote_copy(
            src, pol_out, p_send.at[s], p_recv, device_id={"rep": r + (R >> (s + 1))}, device_id_type=MESH
        )

    @pl.when(r == 0)
    def _():
        for s in range(steps):
            pol(pol_in, s).start()
        pltpu.make_async_copy(pol_in, pol_out, p_loc).start()

    def pol_point(s):
        gap = R >> (s + 1)

        @pl.when(lax.rem(r, 2 * gap) == gap)
        def _():
            pltpu.make_async_copy(pol_out, pol_out, p_recv).wait()
            for q in range(s + 1, steps):
                pol(pol_out, q).start()

    def ag_copy(d, b, c, slot):
        return pltpu.make_async_remote_copy(
            nrm.at[b, c], nrm.at[b, c], ag_send.at[d, slot], ag_recv.at[b, c],
            device_id={"tp": t + (1 if d == 0 else -1)}, device_id_type=MESH,
        )

    def ag_wait(b, c):
        pltpu.make_async_copy(nrm.at[b, c], nrm.at[b, c], ag_recv.at[b, c]).wait()

    def ag_up(i):
        old = i - 2
        jo = jnp.maximum(old, 0) // C

        @pl.when((old >= 0) & (jo <= t) & (t < n - 1))
        def _():
            ag_copy(0, jo, lax.rem(old, C), lax.rem(i, 2)).wait_send()

        j = jnp.maximum(i, 0) // C
        c = lax.rem(jnp.maximum(i, 0), C)

        @pl.when((i >= 0) & (j < t))
        def _():
            ag_wait(j, c)

        @pl.when((i >= 0) & (j <= t) & (t < n - 1))
        def _():
            ag_copy(0, j, c, lax.rem(i, 2)).start()

    def ag_down(i):
        old = i - 2
        bo = t + jnp.maximum(old, 0) // C

        @pl.when((old >= 0) & (bo < n) & (t > 0))
        def _():
            ag_copy(1, bo, lax.rem(jnp.maximum(old, 0), C), lax.rem(i, 2)).wait_send()

        b = t + i // C
        c = lax.rem(i, C)

        @pl.when((b < n) & (t > 0))
        def _():
            @pl.when(b > t)
            def _():
                ag_wait(b, c)

            ag_copy(1, b, c, lax.rem(i, 2)).start()

    def rs_copy(d, b, c, slot):
        dst = b if d == 0 else jnp.where(b == t - 1, n, b)
        return pltpu.make_async_remote_copy(
            part.at[b, c], part.at[dst, c], rs_send.at[d, slot], rs_recv.at[dst, c],
            device_id={"tp": t + (1 if d == 0 else -1)}, device_id_type=MESH,
        )

    def rs_wait(slot, c):
        pltpu.make_async_copy(part.at[slot, c], part.at[slot, c], rs_recv.at[slot, c]).wait()

    def project(b, c):
        return jnp.dot(att[b], wo[c], preferred_element_type=F32).astype(BF16)

    def rs_step(d, i):
        first = 1 if d == 0 else 0

        def live(b):
            return (b < n) & ((b > t) if d == 0 else (b < t))

        old = i - 2
        bo = first + jnp.maximum(old, 0) // C

        @pl.when((old >= 0) & live(bo))
        def _():
            rs_copy(d, bo, lax.rem(jnp.maximum(old, 0), C), lax.rem(i, 2)).wait_send()

        b = first + jnp.maximum(i, 0) // C
        c = lax.rem(jnp.maximum(i, 0), C)
        has = (t > 0) if d == 0 else (t < n - 1)

        @pl.when((i >= 0) & live(b))
        def _():
            mine = project(b, c)

            @pl.when(has)
            def _():
                rs_wait(b, c)
                part[b, c] = (part[b, c].astype(F32) + mine.astype(F32)).astype(BF16)

            @pl.when(jnp.logical_not(has))
            def _():
                part[b, c] = mine

            rs_copy(d, b, c, lax.rem(i, 2)).start()

    group = QH // KVH
    pieces = kvw // HS
    my_head = (t * heads) // group

    def kv_copy(b, p, k):
        target = lax.rem(t + k, n)
        gid = t * pieces + p
        is_v = gid // KVH
        return target, gid, pltpu.make_async_remote_copy(
            kvown.at[p], kvin.at[b, is_v], kv_send.at[p, k], kv_recv.at[b, is_v],
            device_id={"tp": target}, device_id_type=MESH,
        )

    def compute_block(b):
        if b > 0:
            @pl.when(t == 0)
            def _():
                for c in range(C):
                    ag_wait(b, c)

        if b == 0:
            for cp in wloads:
                cp.wait()
        accq[...] = jnp.zeros_like(accq)
        acckv[...] = jnp.zeros_like(acckv)

        def mm(c, carry):
            x = nrm[b, c]
            acckv[...] += jnp.dot(x, wkv[c], preferred_element_type=F32)
            accq[...] += jnp.dot(x, wq[c], preferred_element_type=F32)
            return carry

        lax.fori_loop(0, C, mm, 0)
        for p in range(pieces):
            kvown[p] = acckv[:, p * HS : (p + 1) * HS].astype(BF16)
        for p in range(pieces):
            gid = t * pieces + p
            for k in range(1, n):
                target, _, cp = kv_copy(b, p, k)

                @pl.when(lax.rem(gid, KVH) == (target * heads) // group)
                def _(cp=cp):
                    cp.start()

            here = lax.rem(gid, KVH) == my_head

            @pl.when(here & (gid < KVH))
            def _(p=p):
                kf[b * rows : (b + 1) * rows, :] = kvown[p]

            @pl.when(here & (gid >= KVH))
            def _(p=p):
                vf[b * rows : (b + 1) * rows, :] = kvown[p]

        for h in range(heads):
            qs[h] = accq[:, h * HS : (h + 1) * HS].astype(BF16)
        for is_v, full in ((0, kf), (1, vf)):
            owner = (is_v * KVH + my_head) // pieces

            @pl.when(owner != t)
            def _(is_v=is_v, full=full):
                pltpu.make_async_copy(kvin.at[b, is_v], kvin.at[b, is_v], kv_recv.at[b, is_v]).wait()
                full[b * rows : (b + 1) * rows, :] = kvin[b, is_v]

        span = (b + 1) * rows
        rowpos = b * rows + lax.broadcasted_iota(jnp.int32, (rows, span), 0)
        colpos = lax.broadcasted_iota(jnp.int32, (rows, span), 1)
        valid = (colpos <= rowpos) & (colpos < length)
        for h in range(heads):
            s = lax.dot_general(
                qs[h], kf[:span, :], (((1,), (1,)), ((), ())), preferred_element_type=F32
            ) * HS ** (-0.5)
            s = jnp.where(valid, s, -1e30)
            e = jnp.exp(s - jnp.max(s, axis=1, keepdims=True))
            pr = (e / jnp.sum(e, axis=1, keepdims=True)).astype(BF16)
            att[b, :, h * HS : (h + 1) * HS] = jnp.dot(
                pr, vf[:span, :], preferred_element_type=F32
            ).astype(BF16)
        for p in range(pieces):
            gid = t * pieces + p
            for k in range(1, n):
                target, _, cp = kv_copy(b, p, k)

                @pl.when(lax.rem(gid, KVH) == (target * heads) // group)
                def _(cp=cp):
                    cp.wait_send()

    skew = (n - 1) * LAG
    marks = [(j + 1) * C + skew for j in range(n - 1)]
    up_end = marks[min(1, n - 2)] + (n - 1) * C + skew + 2
    down_end = marks[0] + (n - 1) * C + skew + 2
    up_base = marks[min(1, n - 2)]

    def ag(k):
        ag_down(k)
        ag_up(k - t * LAG)

    def rs_d(k):
        rs_step(1, k - marks[0] - (n - 1 - t) * LAG)

    def rs_u(k):
        rs_step(0, k - up_base - t * LAG)

    def run(lo, hi, fs):
        def body(k, carry):
            for f in fs:
                f(k)
            return carry

        if hi > lo:
            lax.fori_loop(lo, hi, body, 0)

    run(0, marks[0], [ag])
    for b in range(n):
        compute_block(b)
        if b < steps - 1:
            pol_point(b)
        if b == 0:
            for cp in oloads:
                cp.wait()
        if b < n - 2:
            fs = [ag, rs_d]
            if b >= 1:
                fs.append(rs_u)
            run(marks[b], marks[b + 1], fs)
    for s in range(n, steps - 1):
        pol_point(s)
    top = marks[n - 2]
    run(top, top + 2, [ag, rs_u, rs_d])
    run(top + 2, max(up_end, down_end), [rs_u, rs_d])

    local_last = length - 1 - t * rows
    rowid = lax.broadcasted_iota(jnp.int32, (rows, 1), 0)
    weight = jnp.where(rowid == local_last, 1.0, 0.0) + seq ** (-0.5)

    def fin(c, acc):
        total = project(t, c).astype(F32)

        @pl.when(t > 0)
        def _():
            rs_wait(t, c)

        @pl.when(t < n - 1)
        def _():
            rs_wait(n, c)

        below = jnp.where(t > 0, part[t, c].astype(F32), 0.0)
        above = jnp.where(t < n - 1, part[n, c].astype(F32), 0.0)
        hid = (resid[c].astype(F32) + (total + below + above)).astype(BF16)
        resid[c] = hid
        pltpu.make_async_copy(resid.at[c], chunk_of(out_h.at[0], c), out_sem.at[c]).start()
        return acc + jnp.sum(hid.astype(F32) * head[c].astype(F32), axis=1, keepdims=True)

    score = lax.fori_loop(0, C, fin, jnp.zeros((rows, 1), F32))
    rmy[...] = jnp.broadcast_to(jnp.sum(score * weight, keepdims=True), rmy.shape)
    pol_point(steps - 1)

    def rcopy(k):
        return pltpu.make_async_remote_copy(
            rmy, rin.at[k - 1], r_send.at[k - 1], r_recv.at[k - 1],
            device_id={"tp": lax.rem(t + k, n)}, device_id_type=MESH,
        )

    for k in range(1, n):
        rcopy(k).start()
    total = rmy[...]
    for k in range(1, n):
        rcopy(k).wait()
        total = total + rin[k - 1]
    rew[...] = total
    for c in range(C):
        pltpu.make_async_copy(resid.at[c], chunk_of(out_h.at[0], c), out_sem.at[c]).wait()

    @pl.when(r == 0)
    def _():
        for s in range(steps):
            pol(pol_in, s).wait_send()
        pltpu.make_async_copy(pol_in, pol_out, p_loc).wait()

    for s in range(steps - 1):
        gap = R >> (s + 1)

        @pl.when(lax.rem(r, 2 * gap) == gap)
        def _(s=s):
            for q in range(s + 1, steps):
                pol(pol_out, q).wait_send()


def solution(mesh):
    n, R = mesh.shape["tp"], mesh.shape["rep"]

    def on_device(residual_in, norm_gain, w_query, w_keyval, w_out, score_head, lengths, policy_slots):
        rows, width = residual_in.shape[1:]
        qw, kvw = w_query.shape[1], w_keyval.shape[1]
        heads = qw // HS
        C = CHUNKS
        cols = width // C
        sem = pltpu.SemaphoreType.DMA
        vm = pl.BlockSpec(memory_space=pltpu.VMEM)
        hbm = pl.BlockSpec(memory_space=pl.ANY)
        hidden, reward, policy = pl.pallas_call(
            functools.partial(kernel, n, R, kvw, heads),
            out_shape=(
                jax.ShapeDtypeStruct(residual_in.shape, BF16),
                jax.ShapeDtypeStruct((8, 128), F32),
                jax.ShapeDtypeStruct(policy_slots.shape, BF16),
            ),
            in_specs=[hbm, vm, hbm, hbm, hbm, vm, pl.BlockSpec(memory_space=pltpu.SMEM), hbm],
            out_specs=(hbm, vm, hbm),
            scratch_shapes=[
                pltpu.VMEM((C, cols, qw), BF16),
                pltpu.VMEM((C, cols, kvw), BF16),
                pltpu.VMEM((C, qw, cols), BF16),
                pltpu.VMEM((C, rows, cols), BF16),
                pltpu.VMEM((n, C, rows, cols), BF16),
                pltpu.VMEM((n + 1, C, rows, cols), BF16),
                pltpu.VMEM((heads, rows, HS), BF16),
                pltpu.VMEM((rows, qw), F32),
                pltpu.VMEM((rows, kvw), F32),
                pltpu.VMEM((kvw // HS, rows, HS), BF16),
                pltpu.VMEM((n, 2, rows, HS), BF16),
                pltpu.VMEM((n * rows, HS), BF16),
                pltpu.VMEM((n * rows, HS), BF16),
                pltpu.VMEM((n, rows, qw), BF16),
                pltpu.VMEM((8, 128), F32),
                pltpu.VMEM((n - 1, 8, 128), F32),
                sem((2 * C + 2,)),
                sem((2, 2)),
                sem((n, C)),
                sem((2, 2)),
                sem((n + 1, C)),
                sem((kvw // HS, n)),
                sem((n, 2)),
                sem((n - 1,)),
                sem((n - 1,)),
                sem((R.bit_length() - 1,)),
                sem,
                sem,
                sem((C,)),
            ],
            compiler_params=pltpu.CompilerParams(
                collective_id=0, has_side_effects=True, vmem_limit_bytes=67043328
            ),
        )(
            residual_in,
            norm_gain.reshape(C, 1, cols),
            w_query.reshape(C, cols, qw),
            w_keyval.reshape(C, cols, kvw),
            w_out,
            score_head.reshape(C, 1, cols),
            lengths,
            policy_slots,
        )
        return hidden, reward[0, :1], policy

    return jax.shard_map(
        on_device,
        mesh=mesh,
        in_specs=(
            P("rep", "tp", None),
            P(),
            P(None, "tp"),
            P(None, "tp"),
            P("tp", None),
            P(),
            P("rep"),
            P("rep", None, "tp"),
        ),
        out_specs=(P("rep", "tp", None), P("rep"), P("rep", None, "tp")),
        check_vma=False,
    )
```

```python
import functools

import jax
import jax.numpy as jnp
from jax import lax
from jax.experimental import pallas as pl
from jax.experimental.pallas import tpu as pltpu
from jax.sharding import PartitionSpec as P

QH = 32
KVH = 4
HS = 128
MESH = pl.DeviceIdType.MESH
F32 = jnp.float32
BF16 = jnp.bfloat16
CHUNKS = 8
LAG = 3
DEPTH = 6
GO = 0


def kernel(
    n, R, kvw, heads,
    resid_h, gain, wq_h, wkv_h, wo_h, head, lens, pol_in,
    out_h, rew, pol_out,
    wq, wkv, wo, resid, nrm, part, qs, accq, acckv, kvown, kvin, kf, vf, att, rmy, rin,
    load_sem, ag_send, ag_recv, rs_send, rs_recv, kv_send, kv_recv, r_send, r_recv, p_send, p_recv, p_loc, out_sem, go_sem,
):
    t = lax.axis_index("tp")
    r = lax.axis_index("rep")
    C = nrm.shape[1]
    rows, cols = nrm.shape[2], nrm.shape[3]
    seq = n * rows
    length = lens[0]

    def chunk_of(ref, c):
        return ref.at[:, pl.ds(pl.multiple_of(c * cols, cols), cols)]

    loads = [pltpu.make_async_copy(chunk_of(resid_h.at[0], c), resid.at[c], load_sem.at[c]) for c in range(C)]
    wloads = [
        pltpu.make_async_copy(wq_h, wq, load_sem.at[C]),
        pltpu.make_async_copy(wkv_h, wkv, load_sem.at[C + 1]),
    ]
    oloads = [pltpu.make_async_copy(chunk_of(wo_h, c), wo.at[c], load_sem.at[C + 2 + c]) for c in range(C)]
    for cp in loads + wloads + oloads:
        cp.start()
    kf[...] = jnp.zeros_like(kf)
    vf[...] = jnp.zeros_like(vf)

    barrier = pltpu.get_barrier_semaphore()
    for k in range(1, n):
        pl.semaphore_signal(barrier, inc=1, device_id={"tp": lax.rem(t + k, n)}, device_id_type=MESH)
    for k in range(1, R):
        pl.semaphore_signal(barrier, inc=1, device_id={"rep": lax.rem(r + k, R)}, device_id_type=MESH)

    for cp in loads:
        cp.wait()

    def sq(c, acc):
        x = resid[c].astype(F32)
        return acc + jnp.sum(x * x, axis=1, keepdims=True)

    ms = lax.fori_loop(0, C, sq, jnp.zeros((rows, 1), F32))
    scale = lax.rsqrt(ms / (C * cols) + 1e-05)

    def norm(c, carry):
        nrm[t, c] = (resid[c].astype(F32) * scale * gain[c].astype(F32)).astype(BF16)
        return carry

    lax.fori_loop(0, C, norm, 0)
    pl.semaphore_wait(barrier, n - 1 + R - 1)

    steps = R.bit_length() - 1

    def pol(src, s):
        return pltpu.make_async_remote_copy(
            src, pol_out, p_send.at[s], p_recv, device_id={"rep": r + (R >> (s + 1))}, device_id_type=MESH
        )

    @pl.when(r == 0)
    def _():
        for s in range(steps):
            pol(pol_in, s).start()
        pltpu.make_async_copy(pol_in, pol_out, p_loc).start()

    def pol_point(s):
        gap = R >> (s + 1)

        @pl.when(lax.rem(r, 2 * gap) == gap)
        def _():
            pltpu.make_async_copy(pol_out, pol_out, p_recv).wait()
            for q in range(s + 1, steps):
                pol(pol_out, q).start()

    def ag_copy(d, b, c, slot):
        return pltpu.make_async_remote_copy(
            nrm.at[b, c], nrm.at[b, c], ag_send.at[d, slot], ag_recv.at[b, c],
            device_id={"tp": t + (1 if d == 0 else -1)}, device_id_type=MESH,
        )

    def ag_wait(b, c):
        pltpu.make_async_copy(nrm.at[b, c], nrm.at[b, c], ag_recv.at[b, c]).wait()

    def ag_up(i):
        old = i - DEPTH
        jo = jnp.maximum(old, 0) // C

        @pl.when((old >= 0) & (jo <= t) & (t < n - 1))
        def _():
            ag_copy(0, jo, lax.rem(old, C), lax.rem(i, DEPTH)).wait_send()

        j = jnp.maximum(i, 0) // C
        c = lax.rem(jnp.maximum(i, 0), C)

        @pl.when((i >= 0) & (j < t))
        def _():
            ag_wait(j, c)

        @pl.when((i >= 0) & (j <= t) & (t < n - 1))
        def _():
            ag_copy(0, j, c, lax.rem(i, DEPTH)).start()

    def ag_down(i):
        old = i - DEPTH
        bo = t + jnp.maximum(old, 0) // C

        @pl.when((old >= 0) & (bo < n) & (t > 0))
        def _():
            ag_copy(1, bo, lax.rem(jnp.maximum(old, 0), C), lax.rem(i, DEPTH)).wait_send()

        b = t + i // C
        c = lax.rem(i, C)

        @pl.when((b < n) & (t > 0))
        def _():
            @pl.when(b > t)
            def _():
                ag_wait(b, c)

            ag_copy(1, b, c, lax.rem(i, DEPTH)).start()

    def rs_copy(d, b, c, slot):
        dst = b if d == 0 else jnp.where(b == t - 1, n, b)
        return pltpu.make_async_remote_copy(
            part.at[b, c], part.at[dst, c], rs_send.at[d, slot], rs_recv.at[dst, c],
            device_id={"tp": t + (1 if d == 0 else -1)}, device_id_type=MESH,
        )

    def rs_wait(slot, c):
        pltpu.make_async_copy(part.at[slot, c], part.at[slot, c], rs_recv.at[slot, c]).wait()

    def project(b, c):
        return jnp.dot(att[b], wo[c], preferred_element_type=F32).astype(BF16)

    def rs_step(d, i):
        first = 1 if d == 0 else 0

        def live(b):
            return (b < n) & ((b > t) if d == 0 else (b < t))

        old = i - DEPTH
        bo = first + jnp.maximum(old, 0) // C

        @pl.when((old >= 0) & live(bo))
        def _():
            rs_copy(d, bo, lax.rem(jnp.maximum(old, 0), C), lax.rem(i, DEPTH)).wait_send()

        b = first + jnp.maximum(i, 0) // C
        c = lax.rem(jnp.maximum(i, 0), C)
        has = (t > 0) if d == 0 else (t < n - 1)

        @pl.when((i >= 0) & live(b))
        def _():
            mine = project(b, c)

            @pl.when(has)
            def _():
                rs_wait(b, c)
                part[b, c] = (part[b, c].astype(F32) + mine.astype(F32)).astype(BF16)

            @pl.when(jnp.logical_not(has))
            def _():
                part[b, c] = mine

            rs_copy(d, b, c, lax.rem(i, DEPTH)).start()

    group = QH // KVH
    pieces = kvw // HS
    my_head = (t * heads) // group

    def kv_copy(b, p, k):
        target = lax.rem(t + k, n)
        gid = t * pieces + p
        is_v = gid // KVH
        return target, gid, pltpu.make_async_remote_copy(
            kvown.at[p], kvin.at[b, is_v], kv_send.at[p, k], kv_recv.at[b, is_v],
            device_id={"tp": target}, device_id_type=MESH,
        )

    def compute_block(b):
        if b > 0:
            @pl.when(t == 0)
            def _():
                for c in range(C):
                    ag_wait(b, c)

        if b == 0:
            for cp in wloads:
                cp.wait()
        accq[...] = jnp.zeros_like(accq)
        acckv[...] = jnp.zeros_like(acckv)

        def mm(c, carry):
            x = nrm[b, c]
            acckv[...] += jnp.dot(x, wkv[c], preferred_element_type=F32)
            accq[...] += jnp.dot(x, wq[c], preferred_element_type=F32)
            return carry

        lax.fori_loop(0, C, mm, 0)
        for p in range(pieces):
            kvown[p] = acckv[:, p * HS : (p + 1) * HS].astype(BF16)
        for p in range(pieces):
            gid = t * pieces + p
            for k in range(1, n):
                target, _, cp = kv_copy(b, p, k)

                @pl.when(lax.rem(gid, KVH) == (target * heads) // group)
                def _(cp=cp):
                    cp.start()

            here = lax.rem(gid, KVH) == my_head

            @pl.when(here & (gid < KVH))
            def _(p=p):
                kf[b * rows : (b + 1) * rows, :] = kvown[p]

            @pl.when(here & (gid >= KVH))
            def _(p=p):
                vf[b * rows : (b + 1) * rows, :] = kvown[p]

        for h in range(heads):
            qs[h] = accq[:, h * HS : (h + 1) * HS].astype(BF16)
        for is_v, full in ((0, kf), (1, vf)):
            owner = (is_v * KVH + my_head) // pieces

            @pl.when(owner != t)
            def _(is_v=is_v, full=full):
                pltpu.make_async_copy(kvin.at[b, is_v], kvin.at[b, is_v], kv_recv.at[b, is_v]).wait()
                full[b * rows : (b + 1) * rows, :] = kvin[b, is_v]

        span = (b + 1) * rows
        rowpos = b * rows + lax.broadcasted_iota(jnp.int32, (rows, span), 0)
        colpos = lax.broadcasted_iota(jnp.int32, (rows, span), 1)
        valid = (colpos <= rowpos) & (colpos < length)
        for h in range(heads):
            s = lax.dot_general(
                qs[h], kf[:span, :], (((1,), (1,)), ((), ())), preferred_element_type=F32
            ) * HS ** (-0.5)
            s = jnp.where(valid, s, -1e30)
            e = jnp.exp(s - jnp.max(s, axis=1, keepdims=True))
            pr = (e / jnp.sum(e, axis=1, keepdims=True)).astype(BF16)
            att[b, :, h * HS : (h + 1) * HS] = jnp.dot(
                pr, vf[:span, :], preferred_element_type=F32
            ).astype(BF16)
        for p in range(pieces):
            gid = t * pieces + p
            for k in range(1, n):
                target, _, cp = kv_copy(b, p, k)

                @pl.when(lax.rem(gid, KVH) == (target * heads) // group)
                def _(cp=cp):
                    cp.wait_send()

    skew = (n - 1) * LAG
    marks = [(j + 1) * C + skew for j in range(n - 1)]
    up_end = marks[min(1, n - 2)] + (n - 1) * C + skew + DEPTH
    down_end = marks[0] + (n - 1) * C + skew + DEPTH
    up_base = marks[min(1, n - 2)]

    def ag(k):
        ag_down(k)
        ag_up(k - t * LAG)

    def rs_d(k):
        rs_step(1, k - marks[0] - (n - 1 - t) * LAG)

    def rs_u(k):
        rs_step(0, k - up_base - t * LAG)

    def run(lo, hi, fs):
        def body(k, carry):
            for f in fs:
                f(k)
            return carry

        if hi > lo:
            lax.fori_loop(lo, hi, body, 0)

    @pl.when(lax.rem(r, 2) == 1)
    def _():
        pl.semaphore_wait(go_sem, 1)

    run(0, marks[0], [ag])
    for b in range(n):
        if b == min(GO, n - 1):
            @pl.when(lax.rem(r, 2) == 0)
            def _():
                pl.semaphore_signal(go_sem, inc=1, device_id={"rep": r + 1}, device_id_type=MESH)

        compute_block(b)
        if b < steps - 1:
            pol_point(b)
        if b == 0:
            for cp in oloads:
                cp.wait()
        if b < n - 2:
            fs = [ag, rs_d]
            if b >= 1:
                fs.append(rs_u)
            run(marks[b], marks[b + 1], fs)
    for s in range(n, steps - 1):
        pol_point(s)
    top = marks[n - 2]
    run(top, top + DEPTH, [ag, rs_u, rs_d])
    run(top + DEPTH, max(up_end, down_end), [rs_u, rs_d])

    local_last = length - 1 - t * rows
    rowid = lax.broadcasted_iota(jnp.int32, (rows, 1), 0)
    weight = jnp.where(rowid == local_last, 1.0, 0.0) + seq ** (-0.5)

    def fin(c, acc):
        total = project(t, c).astype(F32)

        @pl.when(t > 0)
        def _():
            rs_wait(t, c)

        @pl.when(t < n - 1)
        def _():
            rs_wait(n, c)

        below = jnp.where(t > 0, part[t, c].astype(F32), 0.0)
        above = jnp.where(t < n - 1, part[n, c].astype(F32), 0.0)
        hid = (resid[c].astype(F32) + (total + below + above)).astype(BF16)
        resid[c] = hid
        pltpu.make_async_copy(resid.at[c], chunk_of(out_h.at[0], c), out_sem.at[c]).start()
        return acc + jnp.sum(hid.astype(F32) * head[c].astype(F32), axis=1, keepdims=True)

    score = lax.fori_loop(0, C, fin, jnp.zeros((rows, 1), F32))
    rmy[...] = jnp.broadcast_to(jnp.sum(score * weight, keepdims=True), rmy.shape)
    pol_point(steps - 1)

    def rcopy(k):
        return pltpu.make_async_remote_copy(
            rmy, rin.at[k - 1], r_send.at[k - 1], r_recv.at[k - 1],
            device_id={"tp": lax.rem(t + k, n)}, device_id_type=MESH,
        )

    for k in range(1, n):
        rcopy(k).start()
    total = rmy[...]
    for k in range(1, n):
        rcopy(k).wait()
        total = total + rin[k - 1]
    rew[...] = total
    for c in range(C):
        pltpu.make_async_copy(resid.at[c], chunk_of(out_h.at[0], c), out_sem.at[c]).wait()

    @pl.when(r == 0)
    def _():
        for s in range(steps):
            pol(pol_in, s).wait_send()
        pltpu.make_async_copy(pol_in, pol_out, p_loc).wait()

    for s in range(steps - 1):
        gap = R >> (s + 1)

        @pl.when(lax.rem(r, 2 * gap) == gap)
        def _(s=s):
            for q in range(s + 1, steps):
                pol(pol_out, q).wait_send()


def solution(mesh):
    n, R = mesh.shape["tp"], mesh.shape["rep"]

    def on_device(residual_in, norm_gain, w_query, w_keyval, w_out, score_head, lengths, policy_slots):
        rows, width = residual_in.shape[1:]
        qw, kvw = w_query.shape[1], w_keyval.shape[1]
        heads = qw // HS
        C = CHUNKS
        cols = width // C
        sem = pltpu.SemaphoreType.DMA
        vm = pl.BlockSpec(memory_space=pltpu.VMEM)
        hbm = pl.BlockSpec(memory_space=pl.ANY)
        hidden, reward, policy = pl.pallas_call(
            functools.partial(kernel, n, R, kvw, heads),
            out_shape=(
                jax.ShapeDtypeStruct(residual_in.shape, BF16),
                jax.ShapeDtypeStruct((8, 128), F32),
                jax.ShapeDtypeStruct(policy_slots.shape, BF16),
            ),
            in_specs=[hbm, vm, hbm, hbm, hbm, vm, pl.BlockSpec(memory_space=pltpu.SMEM), hbm],
            out_specs=(hbm, vm, hbm),
            scratch_shapes=[
                pltpu.VMEM((C, cols, qw), BF16),
                pltpu.VMEM((C, cols, kvw), BF16),
                pltpu.VMEM((C, qw, cols), BF16),
                pltpu.VMEM((C, rows, cols), BF16),
                pltpu.VMEM((n, C, rows, cols), BF16),
                pltpu.VMEM((n + 1, C, rows, cols), BF16),
                pltpu.VMEM((heads, rows, HS), BF16),
                pltpu.VMEM((rows, qw), F32),
                pltpu.VMEM((rows, kvw), F32),
                pltpu.VMEM((kvw // HS, rows, HS), BF16),
                pltpu.VMEM((n, 2, rows, HS), BF16),
                pltpu.VMEM((n * rows, HS), BF16),
                pltpu.VMEM((n * rows, HS), BF16),
                pltpu.VMEM((n, rows, qw), BF16),
                pltpu.VMEM((8, 128), F32),
                pltpu.VMEM((n - 1, 8, 128), F32),
                sem((2 * C + 2,)),
                sem((2, DEPTH)),
                sem((n, C)),
                sem((2, DEPTH)),
                sem((n + 1, C)),
                sem((kvw // HS, n)),
                sem((n, 2)),
                sem((n - 1,)),
                sem((n - 1,)),
                sem((R.bit_length() - 1,)),
                sem,
                sem,
                sem((C,)),
                pltpu.SemaphoreType.REGULAR,
            ],
            compiler_params=pltpu.CompilerParams(
                collective_id=0, has_side_effects=True, vmem_limit_bytes=67043328
            ),
        )(
            residual_in,
            norm_gain.reshape(C, 1, cols),
            w_query.reshape(C, cols, qw),
            w_keyval.reshape(C, cols, kvw),
            w_out,
            score_head.reshape(C, 1, cols),
            lengths,
            policy_slots,
        )
        return hidden, reward[0, :1], policy

    return jax.shard_map(
        on_device,
        mesh=mesh,
        in_specs=(
            P("rep", "tp", None),
            P(),
            P(None, "tp"),
            P(None, "tp"),
            P("tp", None),
            P(),
            P("rep"),
            P("rep", None, "tp"),
        ),
        out_specs=(P("rep", "tp", None), P("rep"), P("rep", None, "tp")),
        check_vma=False,
    )
```
